32 devices in a mesh: dp: 16 (over z, y, x), shard: 2 (over core).
Axes of the slice: x: 2, y: 2, z: 4, core: 2. Of those that a mesh axis runs over, the one named last changes fastest.
Arguments:
- features: bfloat16 [65536, 1024], P('dp'), may hold values from -150 to 150
- shared_weight: bfloat16 [1024, 2048], P(None, 'shard'), may hold values from -0.1875 to 0.1875
- task_heads: bfloat16 [6, 2048], P(None, 'shard'), may hold values from -0.4 to 0.4
- labels: int32 [65536, 6], P('dp'), may hold values from 0 to 1
- task_masks: int32 [65536, 6], P('dp'), may hold values from 0 to 1
- task_weights: float32 [6], replicated, may hold values from 0.5 to 2
- initial_losses: float32 [6], replicated, may hold values from 0.2 to 1
Outputs:
- update: float32 [1024, 2048], P('dp', 'shard')
- new_weights: float32 [6], replicated
The draws below stay inside these ranges and needn't reach their ends.
All inputs are finite; a program needn't handle non-finite values.
Results may differ from the reference program's by a relative error of at most 0.00089.
Values sent between devices are 32-bit elements; how exact they have to be, the bound alone decides.
No kernel may reach another device: no remote copies, remote signals or barrier semaphores. Data moves between devices by JAX's collectives and lax.ppermute only.
A program may use at most 256 MiB of HBM per device.

```python
import math
import jax
import jax.numpy as jnp
from jax import lax

DIN = 1024
DH = 2048
TASKS = 6
SAMPLES_DEV = 4096
SAMPLES = 65536
N_DP = 16


def draw_features(key, part):
    subkeys = jax.random.split(key, 3)
    total_rows = SAMPLES_DEV * N_DP
    row_ids = jnp.arange(total_rows)
    column_ids = jnp.arange(DIN)
    roughness = jax.random.uniform(subkeys[1], (DIN,), jnp.float32, -0.5, 0.5)
    column_scale = jnp.exp(math.log(3.0) * column_ids.astype(jnp.float32) / (DIN - 1) + math.log(4.0) * roughness)
    pairing = jax.random.permutation(subkeys[2], N_DP)
    spike_gain = jnp.where(pairing[row_ids // SAMPLES_DEV][:, None] == (column_ids // (DIN // N_DP))[None, :], 3.0, 1.0)
    base_draw = jax.random.truncated_normal(subkeys[0], -4.0, 4.0, (total_rows, DIN), jnp.float32)
    return (base_draw * column_scale[None, :] * spike_gain).astype(jnp.bfloat16)


def draw_task_heads(key, part):
    subkeys = jax.random.split(key, 2)
    column_ids = jnp.arange(DH).astype(jnp.float32)
    roughness = jax.random.uniform(subkeys[1], (DH,), jnp.float32, -0.5, 0.5)
    column_scale = jnp.exp(math.log(3.0) * column_ids / (DH - 1) + math.log(2.0) * roughness)
    base_draw = jax.random.truncated_normal(subkeys[0], -4.0, 4.0, (TASKS, DH), jnp.float32)
    values = base_draw * column_scale[None, :] / math.sqrt(DH)
    return jnp.clip(values, -0.3984375, 0.3984375).astype(jnp.bfloat16)


def draw_task_masks(key, part):
    total_rows = SAMPLES_DEV * N_DP
    row_ids = jnp.arange(total_rows, dtype=jnp.int32)
    threshold = 250 + 500 * row_ids // (total_rows - 1)
    drawn = jax.random.randint(key, (total_rows, TASKS), 0, 1000, dtype=jnp.int32)
    return (drawn < threshold[:, None]).astype(jnp.int32)


def touch_ends(array, stream_key, smallest, high):
    longest = array.shape.index(max(array.shape))
    spots = []
    for shift in (0, 1):
        where = [jax.random.randint(jax.random.fold_in(stream_key, axis), (), 0, length) for axis, length in enumerate(array.shape)]
        where[longest] = (where[longest] + shift) % array.shape[longest]
        spots.append(tuple(where))
    return array.at[spots[0]].set(smallest).at[spots[1]].set(high)


def shard_levels(key, shape, shards, low, top_value):
    gain, own = 1.0, jax.random.fold_in(key, 6)
    for dim, parts in shards:
        steps = jnp.exp(jax.random.uniform(jax.random.fold_in(own, dim), (parts,), jnp.float32, low / len(shards), top_value / len(shards)))
        gain = gain * jnp.repeat(steps, shape[dim] // parts).reshape([-1 if axis == dim else 1 for axis in range(len(shape))])
    return gain


def gaussian(stream_key, extent, deviation, most, shards=(), held_as=jnp.bfloat16):
    loudness = shard_levels(stream_key, extent, shards, -0.22, 0.18) if shards else 1.0
    values = jax.random.normal(stream_key, extent, jnp.float32) * deviation * loudness
    return jnp.minimum(jnp.maximum(values, -most), most).astype(held_as)


def setup_inputs(seed: int = 0) -> dict:
    splits = jax.random.split(jax.random.key(seed), 8)
    features = draw_features(jax.random.fold_in(splits[7], 71), 0)
    shared_weight = gaussian(splits[1], (DIN, DH), DIN ** -0.5, 0.1875, ((1, 2),))
    task_heads = draw_task_heads(jax.random.fold_in(splits[7], 71), 0)
    labels = touch_ends(jax.random.randint(splits[3], (SAMPLES, TASKS), 0, 2), jax.random.fold_in(splits[3], 1), 0, 1).astype(jnp.int32)
    task_masks = draw_task_masks(jax.random.fold_in(splits[7], 71), 0)
    task_weights = jnp.clip(jnp.exp(jax.random.uniform(splits[5], (TASKS,), jnp.float32, math.log(0.5), math.log(2.0))), 0.5, 2.0)
    initial_losses = jnp.clip(jnp.exp(jax.random.uniform(splits[6], (TASKS,), jnp.float32, math.log(0.2), math.log(1.0))), 0.2, 1.0)
    return dict(features=features, shared_weight=shared_weight, task_heads=task_heads, labels=labels, task_masks=task_masks, task_weights=task_weights, initial_losses=initial_losses)


epsilon = 1e-06
learn_rate = 0.5
asymmetry = 1.5

def silu_parts(preact):
    sigmoid_pre = jax.nn.sigmoid(preact)
    return (preact * sigmoid_pre, sigmoid_pre * (1.0 + preact * (1.0 - sigmoid_pre)))

def renew_weights(losses, squares, task_weights, initial_losses, entries):
    root_mean = jnp.sqrt(squares / entries + epsilon)
    scaled = task_weights * root_mean
    average = jnp.mean(scaled)
    loss_ratio = losses / initial_losses
    relative = loss_ratio / jnp.mean(loss_ratio)
    target = average * relative ** asymmetry
    distance = (scaled - target) / average
    raised = task_weights * jnp.exp(-learn_rate * distance)
    return raised.shape[0] * raised / jnp.sum(raised)

def reference(features, shared_weight, task_heads, labels, task_masks, task_weights, initial_losses):
    blocks = features.reshape(N_DP, SAMPLES_DEV, DIN)
    label_blocks = labels.reshape(N_DP, SAMPLES_DEV, TASKS)
    mask_blocks = task_masks.reshape(N_DP, SAMPLES_DEV, TASKS)
    heads_wide = task_heads.astype(jnp.float32)

    def block_step(running, inputs):
        grad_sum, loss_sum = running
        rows_in, label_rows, mask_rows = inputs
        preact = jnp.dot(rows_in, shared_weight, preferred_element_type=jnp.float32)
        activated, silu_slope = silu_parts(preact)
        hidden = activated.astype(jnp.bfloat16)
        logits = jnp.dot(hidden, task_heads.T, preferred_element_type=jnp.float32)
        targets = label_rows.astype(jnp.float32)
        mask_float = mask_rows.astype(jnp.float32)
        loss_sum = loss_sum + lax.optimization_barrier(jnp.sum(mask_float * (jax.nn.softplus(logits) - targets * logits), axis=0))
        errors = mask_float * (jax.nn.sigmoid(logits) - targets)
        back_terms = (errors[:, :, None] * silu_slope[:, None, :] * heads_wide[None]).astype(jnp.bfloat16)
        back_flat = back_terms.reshape(SAMPLES_DEV, TASKS * DH)
        grad_sum = grad_sum + lax.dot_general(rows_in, back_flat, (((0,), (0,)), ((), ())), preferred_element_type=jnp.float32)
        return ((grad_sum, loss_sum), None)
    start_state = (jnp.zeros((DIN, TASKS * DH), jnp.float32), jnp.zeros((TASKS,), jnp.float32))
    (grad_sum, loss_sum), unused = lax.scan(block_step, start_state, (blocks, label_blocks, mask_blocks))
    gradients = grad_sum.reshape(DIN, TASKS, DH)
    losses = loss_sum / SAMPLES
    squares = lax.optimization_barrier(jnp.sum(gradients * gradients, axis=(0, 2)))
    new_weights = renew_weights(losses, squares, task_weights, initial_losses, DIN * DH)
    combined = jnp.einsum('t,rtc->rc', new_weights, gradients, precision=lax.Precision.HIGHEST)
    update = combined * lax.rsqrt(jnp.mean(combined * combined) + epsilon)
    return (update, new_weights)
```

```python
import functools
import jax
import jax.numpy as jnp
from jax import lax
from jax.experimental import pallas as pl
from jax.experimental.pallas import tpu as pltpu
from jax.sharding import PartitionSpec as P

epsilon = 1e-06
learn_rate = 0.5
LANES = 128
SUBLANES = 8
MIB = 1 << 20


def xor_pairs(count, bit):
    return [(place, place ^ (1 << bit)) for place in range(count)]


def split_orders(bits, tasks):
    if bits == 4:
        base = [tuple(int(letter) for letter in name) for name in SPLITS]
    else:
        base = [tuple((start + step) % bits for step in range(bits)) for start in range(bits)]
    return [base[task % len(base)] for task in range(tasks)]


SPLITS = ("1023", "0123", "2103", "1023", "0123", "2013")


def front_body(place_ref, x_ref, w_ref, heads_ref, slope_ref, logits_ref, turned_ref):
    place = place_ref[0]
    rows = turned_ref.shape[1]
    x = x_ref[...]
    block = x.shape[0]
    here = pl.ds(pl.multiple_of(pl.program_id(0) * block, block), block)
    preact = jnp.dot(x, w_ref[...], preferred_element_type=jnp.float32)
    sigmoid_pre = jax.nn.sigmoid(preact)
    slope_ref[here] = sigmoid_pre * (1.0 + preact * (1.0 - sigmoid_pre))
    hidden = (preact * sigmoid_pre).astype(jnp.bfloat16)
    partial = lax.dot_general(
        hidden, heads_ref[...], (((1,), (1,)), ((), ())), preferred_element_type=jnp.float32
    )
    logits_ref[:, here] = partial.T[:SUBLANES]
    for tile in range(x.shape[1] // LANES):
        turned = x[:, tile * LANES : (tile + 1) * LANES].T
        for part in range(LANES // rows):
            spot = jnp.bitwise_xor(place, tile * (LANES // rows) + part)
            turned_ref[spot, :, here] = turned[part * rows : (part + 1) * rows]


def front(place, features, shared_weight, heads, replicas, block=512):
    samples, width_in = features.shape
    local_hidden = shared_weight.shape[1]
    rows = width_in // replicas
    resident = pl.BlockSpec(memory_space=pltpu.VMEM)
    return pl.pallas_call(
        front_body,
        grid_spec=pltpu.PrefetchScalarGridSpec(
            num_scalar_prefetch=1,
            grid=(samples // block,),
            in_specs=[pl.BlockSpec((block, width_in), lambda i, p: (i, 0)), resident, resident],
            out_specs=[resident, resident, resident],
        ),
        out_shape=[
            pltpu.VMEM((samples, local_hidden), jnp.float32),
            jax.ShapeDtypeStruct((SUBLANES, samples), jnp.float32),
            pltpu.VMEM((replicas, rows, samples), jnp.bfloat16),
        ],
        cost_estimate=pl.CostEstimate(
            flops=2 * samples * width_in * local_hidden,
            bytes_accessed=samples * width_in * 2,
            transcendentals=samples * local_hidden,
        ),
        compiler_params=pltpu.CompilerParams(vmem_limit_bytes=20 * MIB),
        name="front",
    )(place, features, shared_weight, heads)


def errors_body(
    total_samples, one_ref, two_ref, labels_ref, masks_ref, _turned, _slope, errors_ref, losses_ref, *_held
):
    tasks = labels_ref.shape[0]
    logits = (one_ref[...] + two_ref[...])[:tasks]
    targets = labels_ref[...].astype(jnp.float32)
    masks = masks_ref[...].astype(jnp.float32)
    errors_ref[...] = jnp.zeros_like(errors_ref)
    errors_ref[:tasks] = masks * (jax.nn.sigmoid(logits) - targets)
    softplus = jnp.maximum(logits, 0.0) + jnp.log1p(jnp.exp(-jnp.abs(logits)))
    losses = masks * (softplus - targets * logits) / total_samples
    losses_ref[...] = jnp.zeros_like(losses_ref)
    losses_ref[:tasks] = jnp.broadcast_to(
        jnp.sum(losses, axis=1, keepdims=True), (tasks, LANES)
    )


def task_errors(one, two, labels, masks, turned, slope, total_samples):
    resident = pl.BlockSpec(memory_space=pltpu.VMEM)
    return pl.pallas_call(
        functools.partial(errors_body, total_samples),
        in_specs=[resident] * 6,
        out_specs=[resident] * 4,
        out_shape=[
            jax.ShapeDtypeStruct(one.shape, jnp.float32),
            jax.ShapeDtypeStruct((SUBLANES, LANES), jnp.float32),
            pltpu.VMEM(turned.shape, turned.dtype),
            pltpu.VMEM(slope.shape, slope.dtype),
        ],
        input_output_aliases={4: 2, 5: 3},
        compiler_params=pltpu.CompilerParams(vmem_limit_bytes=8 * MIB),
        name="errors",
    )(one, two, labels, masks, turned, slope)


def task_body(
    order, task, wide, turned_ref, slope_ref, errors_ref, heads_ref, send_ref, keep_ref, *rest
):
    terms = rest[-1]
    blocks, rows, depth = turned_ref.shape
    head = heads_ref[task : task + 1].astype(jnp.float32)
    size = min(1024, depth)

    def fill(piece, carry):
        here = pl.ds(pl.multiple_of(piece * size, size), size)
        column = errors_ref[:, here].T[:, task : task + 1]
        terms[here] = ((column * slope_ref[here]) * head).astype(jnp.bfloat16)
        return carry

    lax.fori_loop(0, depth // size, fill, 0)
    ranked = sorted(range(blocks), key=lambda block: [block >> bit & 1 for bit in order])
    half = blocks // 2

    def multiply(tile, carry):
        columns = pl.ds(pl.multiple_of(tile * wide, wide), wide)
        product = jnp.dot(
            turned_ref[...].reshape(blocks * rows, depth),
            terms[:, columns],
            preferred_element_type=jnp.float32,
        )
        for block in range(blocks):
            spot = ranked.index(block)
            out = keep_ref if spot < half else send_ref
            place = pl.ds(spot % half * rows, rows)
            out[place, columns] = product[block * rows : (block + 1) * rows]
        return carry

    lax.fori_loop(0, terms.shape[1] // wide, multiply, 0)


def task_terms(task, order, turned, slope, errors, heads, wide=256):
    blocks, rows, samples = turned.shape
    width = slope.shape[1]
    half = jax.ShapeDtypeStruct((blocks // 2 * rows, width), jnp.float32)
    resident = pl.BlockSpec(memory_space=pltpu.VMEM)
    return pl.pallas_call(
        functools.partial(task_body, order, task, wide),
        in_specs=[resident] * 4,
        out_specs=[resident] * 4,
        out_shape=[
            half,
            half,
            pltpu.VMEM(turned.shape, turned.dtype),
            pltpu.VMEM(slope.shape, slope.dtype),
        ],
        input_output_aliases={0: 2, 1: 3},
        scratch_shapes=[pltpu.VMEM((samples, width), jnp.bfloat16)],
        cost_estimate=pl.CostEstimate(
            flops=2 * samples * blocks * rows * width,
            bytes_accessed=samples * LANES * 4,
            transcendentals=0,
        ),
        compiler_params=pltpu.CompilerParams(vmem_limit_bytes=16 * MIB),
        name="task",
    )(turned, slope, errors, heads)


def gram_body(tasks, *refs):
    keeps, arrived, losses_ref = refs[:tasks], refs[tasks : 2 * tasks], refs[2 * tasks]
    gradients, packed_ref = refs[2 * tasks + 1 : -1], refs[-1]
    rows, width = keeps[0].shape
    pairs = [(one, two) for one in range(tasks) for two in range(one, tasks)]
    zeros = jnp.zeros((SUBLANES, LANES), jnp.float32)

    def strip(index, sums):
        here = pl.ds(pl.multiple_of(index * SUBLANES, SUBLANES), SUBLANES)
        values = []
        for task in range(tasks):
            value = keeps[task][here] + arrived[task][here]
            gradients[task][here] = value
            values.append(value)
        out = []
        for (one, two), total in zip(pairs, sums):
            product = values[one] * values[two]
            for tile in range(width // LANES):
                total = total + product[:, tile * LANES : (tile + 1) * LANES]
            out.append(total)
        return tuple(out)

    sums = lax.fori_loop(0, rows // SUBLANES, strip, (zeros,) * len(pairs))
    row = lax.broadcasted_iota(jnp.int32, (SUBLANES, LANES), 0)
    lane = lax.broadcasted_iota(jnp.int32, (SUBLANES, LANES), 1)
    packed = zeros
    for (one, two), total in zip(pairs, sums):
        value = jnp.sum(total, keepdims=True)
        spots = ((row == one) & (lane == two)) | ((row == two) & (lane == one))
        if one == two:
            spots = spots | ((row == tasks + 1) & (lane == one))
        packed = jnp.where(spots, value, packed)
    for task in range(tasks):
        value = losses_ref[task : task + 1, :1]
        packed = jnp.where((row == tasks) & (lane == task), value, packed)
    packed_ref[...] = jnp.broadcast_to(packed[None], packed_ref.shape)


def gram_terms(keeps, arrived, losses, devices):
    tasks = len(keeps)
    piece = jax.ShapeDtypeStruct(keeps[0].shape, jnp.float32)
    resident = pl.BlockSpec(memory_space=pltpu.VMEM)
    found = pl.pallas_call(
        functools.partial(gram_body, tasks),
        in_specs=[resident] * (2 * tasks + 1),
        out_specs=[resident] * (tasks + 1),
        out_shape=[piece] * tasks
        + [jax.ShapeDtypeStruct((devices, SUBLANES, LANES), jnp.float32)],
        compiler_params=pltpu.CompilerParams(vmem_limit_bytes=16 * MIB),
        name="gram",
    )(*keeps, *arrived, losses)
    return found[:-1], found[-1]


def final_body(tasks, entries, shards, shared_ref, weights_ref, initial_ref, *refs):
    gradients, update_ref, fresh_ref = refs[:tasks], refs[-2], refs[-1]
    total = jnp.sum(shared_ref[...], axis=0)
    lane = lax.broadcasted_iota(jnp.int32, (1, LANES), 1)
    live = lane < tasks
    losses = total[tasks : tasks + 1] / shards
    squares = total[tasks + 1 : tasks + 2]
    weights = weights_ref[...]
    root_mean = jnp.sqrt(squares / entries + epsilon)
    scaled = weights * root_mean
    average = jnp.sum(jnp.where(live, scaled, 0.0), axis=1, keepdims=True) / tasks
    loss_ratio = losses / initial_ref[...]
    relative = loss_ratio / (
        jnp.sum(jnp.where(live, loss_ratio, 0.0), axis=1, keepdims=True) / tasks
    )
    target = average * (relative * jnp.sqrt(relative))
    distance = (scaled - target) / average
    raised = jnp.where(live, weights * jnp.exp(-learn_rate * distance), 0.0)
    fresh = tasks * raised / jnp.sum(raised, axis=1, keepdims=True)
    inner = jnp.sum(total * fresh, axis=1, keepdims=True)
    each = [fresh[:, task : task + 1] for task in range(tasks)]
    mean_square = sum(each[task] * inner[task : task + 1] for task in range(tasks)) / entries
    scale = lax.rsqrt(mean_square + epsilon)
    combined = each[0] * gradients[0][...]
    for task in range(1, tasks):
        combined = combined + each[task] * gradients[task][...]
    update_ref[...] = combined * scale
    fresh_ref[...] = jnp.broadcast_to(fresh, fresh_ref.shape)


def final_terms(shared, weights, initial, gradients, entries, shards):
    tasks = len(gradients)
    resident = pl.BlockSpec(memory_space=pltpu.VMEM)
    spare = ((0, 0), (0, LANES - tasks))
    return pl.pallas_call(
        functools.partial(final_body, tasks, entries, shards),
        in_specs=[resident] * (3 + tasks),
        out_specs=[resident] * 2,
        out_shape=[
            jax.ShapeDtypeStruct(gradients[0].shape, jnp.float32),
            jax.ShapeDtypeStruct((SUBLANES, LANES), jnp.float32),
        ],
        compiler_params=pltpu.CompilerParams(vmem_limit_bytes=16 * MIB),
        name="final",
    )(
        shared,
        jnp.pad(weights[None], spare, constant_values=1.0),
        jnp.pad(initial[None], spare, constant_values=1.0),
        *gradients,
    )


def on_device(
    features, shared_weight, task_heads, labels, task_masks, task_weights, initial_losses
):
    shard_count = lax.axis_size("shard")
    replica_count = lax.axis_size("dp")
    sample_count, width_in = features.shape
    local_hidden = shared_weight.shape[1]
    task_count = task_heads.shape[0]
    entries = width_in * local_hidden * shard_count
    total_samples = sample_count * replica_count
    bits = replica_count.bit_length() - 1
    heads = jnp.pad(task_heads, ((0, LANES - task_count), (0, 0)))
    place = lax.axis_index("dp").astype(jnp.int32).reshape(1)
    slope, logits, turned = front(place, pltpu.with_memory_space_constraint(features, pltpu.HBM), shared_weight, heads, replica_count)
    received = jnp.zeros_like(logits)
    for bit in range(shard_count.bit_length() - 1):
        logits = logits + received if bit else logits
        received = lax.ppermute(logits, "shard", xor_pairs(shard_count, bit))
    errors, losses, turned, slope = task_errors(
        logits, received, labels.T, task_masks.T, turned, slope, total_samples
    )
    keeps, arrived = [], []
    for task, order in enumerate(split_orders(bits, task_count)):
        send, keep, turned, slope = task_terms(task, order, turned, slope, errors, heads)
        for step, bit in enumerate(order):
            received = lax.ppermute(send, "dp", xor_pairs(replica_count, bit))
            if step < bits - 1:
                half = keep.shape[0] // 2
                send = keep[half:] + received[half:]
                keep = keep[:half] + received[:half]
        keeps.append(keep)
        arrived.append(received)
    devices = replica_count * shard_count
    gradients, packed = gram_terms(keeps, arrived, losses, devices)
    shared = lax.all_to_all(packed, ("dp", "shard"), 0, 0)
    update, fresh = final_terms(
        shared, task_weights, initial_losses, gradients, entries, shard_count
    )
    return (update, fresh[0, :task_count])


def solution(mesh):
    return jax.shard_map(
        on_device,
        mesh=mesh,
        in_specs=(
            P("dp", None),
            P(None, "shard"),
            P(None, "shard"),
            P("dp", None),
            P("dp", None),
            P(),
            P(),
        ),
        out_specs=(P("dp", "shard"), P()),
        check_vma=False,
    )
```

```python
import functools
import jax
import jax.numpy as jnp
from jax import lax
from jax.experimental import pallas as pl
from jax.experimental.pallas import tpu as pltpu
from jax.sharding import PartitionSpec as P

epsilon = 1e-06
learn_rate = 0.5
LANES = 128
SUBLANES = 8
MIB = 1 << 20


def xor_pairs(count, bit):
    return [(place, place ^ (1 << bit)) for place in range(count)]


PARTS = (3, 2, 3, 4, 2, 3, 2, 2, 2, 1)
SPLITS = ("2013", "1203", "0213", "1203", "2013", "0123", "1203", "0213", "1023", "2103")


def split_work(bits, tasks, width):
    unit = tasks * width // sum(PARTS)
    if bits == 4 and unit % (2 * LANES) == 0 and unit * sum(PARTS) == tasks * width:
        counts = [part * unit for part in PARTS]
        orders = [tuple(int(letter) for letter in name) for name in SPLITS]
    else:
        counts = [width] * tasks
        orders = [tuple((task + step) % bits for step in range(bits)) for task in range(tasks)]
    return [(sum(counts[:spot]), counts[spot], orders[spot]) for spot in range(len(counts))]


def front_body(place_ref, x_ref, w_ref, heads_ref, slope_ref, logits_ref, turned_ref, padded):
    place = place_ref[0]

    @pl.when(pl.program_id(0) == 0)
    def _():
        padded[...] = jnp.zeros_like(padded)
        padded[: heads_ref.shape[0]] = heads_ref[...]

    rows = turned_ref.shape[1]
    x = x_ref[...]
    block = x.shape[0]
    here = pl.ds(pl.multiple_of(pl.program_id(0) * block, block), block)
    preact = jnp.dot(x, w_ref[...], preferred_element_type=jnp.float32)
    sigmoid_pre = jax.nn.sigmoid(preact)
    slope_ref[here] = sigmoid_pre * (1.0 + preact * (1.0 - sigmoid_pre))
    hidden = (preact * sigmoid_pre).astype(jnp.bfloat16)
    partial = lax.dot_general(
        hidden, padded[...], (((1,), (1,)), ((), ())), preferred_element_type=jnp.float32
    )
    logits_ref[:, here] = partial.T[:SUBLANES]
    for tile in range(x.shape[1] // LANES):
        turned = x[:, tile * LANES : (tile + 1) * LANES].T
        for part in range(LANES // rows):
            spot = jnp.bitwise_xor(place, tile * (LANES // rows) + part)
            turned_ref[spot, :, here] = turned[part * rows : (part + 1) * rows]


def front(place, features, shared_weight, heads, replicas, block=512):
    samples, width_in = features.shape
    local_hidden = shared_weight.shape[1]
    rows = width_in // replicas
    resident = pl.BlockSpec(memory_space=pltpu.VMEM)
    return pl.pallas_call(
        front_body,
        grid_spec=pltpu.PrefetchScalarGridSpec(
            num_scalar_prefetch=1,
            grid=(samples // block,),
            in_specs=[
                pl.BlockSpec((block, width_in), lambda i, p: (i, 0)),
                pl.BlockSpec((width_in, local_hidden), lambda i, p: (0, 0)),
                pl.BlockSpec(heads.shape, lambda i, p: (0, 0)),
            ],
            out_specs=[resident, resident, resident],
            scratch_shapes=[pltpu.VMEM((LANES, local_hidden), jnp.bfloat16)],
        ),
        out_shape=[
            pltpu.VMEM((samples, local_hidden), jnp.float32),
            jax.ShapeDtypeStruct((SUBLANES, samples), jnp.float32),
            pltpu.VMEM((replicas, rows, samples), jnp.bfloat16),
        ],
        cost_estimate=pl.CostEstimate(
            flops=2 * samples * width_in * local_hidden,
            bytes_accessed=samples * width_in * 2,
            transcendentals=samples * local_hidden,
        ),
        compiler_params=pltpu.CompilerParams(vmem_limit_bytes=20 * MIB),
        name="front",
    )(place, features, shared_weight, heads)


def errors_body(
    total_samples, one_ref, two_ref, labels_ref, masks_ref, _turned, _slope, errors_ref, losses_ref, *_held
):
    tasks = labels_ref.shape[0]
    logits = (one_ref[...] + two_ref[...])[:tasks]
    targets = labels_ref[...].astype(jnp.float32)
    masks = masks_ref[...].astype(jnp.float32)
    errors_ref[...] = jnp.zeros_like(errors_ref)
    errors_ref[:tasks] = masks * (jax.nn.sigmoid(logits) - targets)
    softplus = jnp.maximum(logits, 0.0) + jnp.log1p(jnp.exp(-jnp.abs(logits)))
    losses = masks * (softplus - targets * logits) / total_samples
    losses_ref[...] = jnp.zeros_like(losses_ref)
    losses_ref[:tasks] = jnp.broadcast_to(
        jnp.sum(losses, axis=1, keepdims=True), (tasks, LANES)
    )


def task_errors(one, two, labels, masks, turned, slope, total_samples):
    resident = pl.BlockSpec(memory_space=pltpu.VMEM)
    return pl.pallas_call(
        functools.partial(errors_body, total_samples),
        in_specs=[resident] * 6,
        out_specs=[resident] * 4,
        out_shape=[
            jax.ShapeDtypeStruct(one.shape, jnp.float32),
            jax.ShapeDtypeStruct((SUBLANES, LANES), jnp.float32),
            pltpu.VMEM(turned.shape, turned.dtype),
            pltpu.VMEM(slope.shape, slope.dtype),
        ],
        input_output_aliases={4: 2, 5: 3},
        compiler_params=pltpu.CompilerParams(vmem_limit_bytes=8 * MIB),
        name="errors",
    )(one, two, labels, masks, turned, slope)


def segments_of(start, count, width):
    runs, column = [], start
    while column < start + count:
        task, offset = divmod(column, width)
        size = min(width - offset, start + count - column)
        runs.append((task, offset, size, column - start))
        column += size
    return runs


def chunk_body(
    order, runs, wide, turned_ref, slope_ref, errors_ref, heads_ref, send_ref, keep_ref, *rest
):
    terms = rest[-1]
    blocks, rows, depth = turned_ref.shape
    size = min(1024, depth)
    heads = heads_ref[...].astype(jnp.float32)

    def fill(piece, carry):
        here = pl.ds(pl.multiple_of(piece * size, size), size)
        columns = errors_ref[:, here].T
        for task, offset, count, spot in runs:
            scaled = columns[:, task : task + 1] * slope_ref[here, offset : offset + count]
            head = heads[task : task + 1, offset : offset + count]
            terms[here, spot : spot + count] = (scaled * head).astype(jnp.bfloat16)
        return carry

    lax.fori_loop(0, depth // size, fill, 0)
    ranked = sorted(range(blocks), key=lambda block: [block >> bit & 1 for bit in order])
    half = blocks // 2

    def multiply(tile, carry):
        columns = pl.ds(pl.multiple_of(tile * wide, wide), wide)
        product = jnp.dot(
            turned_ref[...].reshape(blocks * rows, depth),
            terms[:, columns],
            preferred_element_type=jnp.float32,
        )
        for block in range(blocks):
            spot = ranked.index(block)
            out = keep_ref if spot < half else send_ref
            place = pl.ds(spot % half * rows, rows)
            out[place, columns] = product[block * rows : (block + 1) * rows]
        return carry

    lax.fori_loop(0, terms.shape[1] // wide, multiply, 0)


def chunk_terms(start, count, order, turned, slope, errors, heads, wide=256):
    blocks, rows, samples = turned.shape
    half = jax.ShapeDtypeStruct((blocks // 2 * rows, count), jnp.float32)
    resident = pl.BlockSpec(memory_space=pltpu.VMEM)
    return pl.pallas_call(
        functools.partial(chunk_body, order, segments_of(start, count, slope.shape[1]), wide),
        in_specs=[resident] * 4,
        out_specs=[resident] * 4,
        out_shape=[
            half,
            half,
            pltpu.VMEM(turned.shape, turned.dtype),
            pltpu.VMEM(slope.shape, slope.dtype),
        ],
        input_output_aliases={0: 2, 1: 3},
        scratch_shapes=[pltpu.VMEM((samples, count), jnp.bfloat16)],
        cost_estimate=pl.CostEstimate(
            flops=2 * samples * blocks * rows * count,
            bytes_accessed=samples * LANES * 4,
            transcendentals=0,
        ),
        compiler_params=pltpu.CompilerParams(vmem_limit_bytes=14 * MIB),
        name="chunk",
    )(turned, slope, errors, heads)


def gram_body(tasks, spots, *refs):
    chunks = (len(refs) - 2 - tasks) // 2
    keeps, arrived, losses_ref = refs[:chunks], refs[chunks : 2 * chunks], refs[2 * chunks]
    gradients, packed_ref = refs[2 * chunks + 1 : -1], refs[-1]
    rows = keeps[0].shape[0]
    pairs = [(one, two) for one in range(tasks) for two in range(one, tasks)]
    zeros = jnp.zeros((SUBLANES, LANES), jnp.float32)

    def strip(index, sums):
        here = pl.ds(pl.multiple_of(index * SUBLANES, SUBLANES), SUBLANES)
        for tile, places in enumerate(spots):
            values = []
            for task, (chunk, offset) in enumerate(places):
                there = slice(offset, offset + LANES)
                value = keeps[chunk][here, there] + arrived[chunk][here, there]
                gradients[task][here, tile * LANES : (tile + 1) * LANES] = value
                values.append(value)
            sums = tuple(
                total + values[one] * values[two] for (one, two), total in zip(pairs, sums)
            )
        return sums

    sums = lax.fori_loop(0, rows // SUBLANES, strip, (zeros,) * len(pairs))
    row = lax.broadcasted_iota(jnp.int32, (SUBLANES, LANES), 0)
    lane = lax.broadcasted_iota(jnp.int32, (SUBLANES, LANES), 1)
    packed = zeros
    for (one, two), total in zip(pairs, sums):
        value = jnp.sum(total, keepdims=True)
        match = ((row == one) & (lane == two)) | ((row == two) & (lane == one))
        if one == two:
            match = match | ((row == tasks + 1) & (lane == one))
        packed = jnp.where(match, value, packed)
    for task in range(tasks):
        value = losses_ref[task : task + 1, :1]
        packed = jnp.where((row == tasks) & (lane == task), value, packed)
    packed_ref[...] = jnp.broadcast_to(packed[None], packed_ref.shape)


def gram_terms(keeps, arrived, losses, work, tasks, width, devices):
    def place(column):
        chunk = max(spot for spot, (start, _, _) in enumerate(work) if start <= column)
        return chunk, column - work[chunk][0]

    spots = [
        [place(task * width + tile * LANES) for task in range(tasks)]
        for tile in range(width // LANES)
    ]
    piece = jax.ShapeDtypeStruct((keeps[0].shape[0], width), jnp.float32)
    resident = pl.BlockSpec(memory_space=pltpu.VMEM)
    found = pl.pallas_call(
        functools.partial(gram_body, tasks, spots),
        in_specs=[resident] * (2 * len(work) + 1),
        out_specs=[resident] * (tasks + 1),
        out_shape=[piece] * tasks
        + [jax.ShapeDtypeStruct((devices, SUBLANES, LANES), jnp.float32)],
        compiler_params=pltpu.CompilerParams(vmem_limit_bytes=16 * MIB),
        name="gram",
    )(*keeps, *arrived, losses)
    return found[:-1], found[-1]


def final_body(tasks, entries, shards, shared_ref, weights_ref, initial_ref, *refs):
    gradients, update_ref, fresh_ref = refs[:tasks], refs[-2], refs[-1]
    total = jnp.sum(shared_ref[...], axis=0)
    lane = lax.broadcasted_iota(jnp.int32, (1, LANES), 1)
    live = lane < tasks
    losses = total[tasks : tasks + 1] / shards
    squares = total[tasks + 1 : tasks + 2]
    weights = weights_ref[...]
    root_mean = jnp.sqrt(squares / entries + epsilon)
    scaled = weights * root_mean
    average = jnp.sum(jnp.where(live, scaled, 0.0), axis=1, keepdims=True) / tasks
    loss_ratio = losses / initial_ref[...]
    relative = loss_ratio / (
        jnp.sum(jnp.where(live, loss_ratio, 0.0), axis=1, keepdims=True) / tasks
    )
    target = average * (relative * jnp.sqrt(relative))
    distance = (scaled - target) / average
    raised = jnp.where(live, weights * jnp.exp(-learn_rate * distance), 0.0)
    fresh = tasks * raised / jnp.sum(raised, axis=1, keepdims=True)
    inner = jnp.sum(total * fresh, axis=1, keepdims=True)
    each = [fresh[:, task : task + 1] for task in range(tasks)]
    mean_square = sum(each[task] * inner[task : task + 1] for task in range(tasks)) / entries
    scale = lax.rsqrt(mean_square + epsilon)
    combined = each[0] * gradients[0][...]
    for task in range(1, tasks):
        combined = combined + each[task] * gradients[task][...]
    update_ref[...] = combined * scale
    fresh_ref[...] = jnp.broadcast_to(fresh, fresh_ref.shape)


def final_terms(shared, weights, initial, gradients, entries, shards):
    tasks = len(gradients)
    resident = pl.BlockSpec(memory_space=pltpu.VMEM)
    spare = ((0, 0), (0, LANES - tasks))
    return pl.pallas_call(
        functools.partial(final_body, tasks, entries, shards),
        in_specs=[resident] * (3 + tasks),
        out_specs=[resident] * 2,
        out_shape=[
            jax.ShapeDtypeStruct(gradients[0].shape, jnp.float32),
            jax.ShapeDtypeStruct((SUBLANES, LANES), jnp.float32),
        ],
        compiler_params=pltpu.CompilerParams(vmem_limit_bytes=16 * MIB),
        name="final",
    )(
        shared,
        jnp.pad(weights[None], spare, constant_values=1.0),
        jnp.pad(initial[None], spare, constant_values=1.0),
        *gradients,
    )


def on_device(
    features, shared_weight, task_heads, labels, task_masks, task_weights, initial_losses
):
    shard_count = lax.axis_size("shard")
    replica_count = lax.axis_size("dp")
    sample_count, width_in = features.shape
    local_hidden = shared_weight.shape[1]
    task_count = task_heads.shape[0]
    entries = width_in * local_hidden * shard_count
    total_samples = sample_count * replica_count
    bits = replica_count.bit_length() - 1
    place = lax.axis_index("dp").astype(jnp.int32).reshape(1)
    slope, logits, turned = front(
        place,
        pltpu.with_memory_space_constraint(features, pltpu.HBM),
        pltpu.with_memory_space_constraint(shared_weight, pltpu.HBM),
        task_heads,
        replica_count,
    )
    received = jnp.zeros_like(logits)
    for bit in range(shard_count.bit_length() - 1):
        logits = logits + received if bit else logits
        received = lax.ppermute(logits, "shard", xor_pairs(shard_count, bit))
    errors, losses, turned, slope = task_errors(
        logits, received, labels.T, task_masks.T, turned, slope, total_samples
    )
    work = split_work(bits, task_count, local_hidden)
    keeps, arrived = [], []
    for start, count, order in work:
        send, keep, turned, slope = chunk_terms(
            start, count, order, turned, slope, errors, task_heads
        )
        for step, bit in enumerate(order):
            received = lax.ppermute(send, "dp", xor_pairs(replica_count, bit))
            if step < bits - 1:
                half = keep.shape[0] // 2
                send = keep[half:] + received[half:]
                keep = keep[:half] + received[:half]
        keeps.append(keep)
        arrived.append(received)
    devices = replica_count * shard_count
    gradients, packed = gram_terms(
        keeps, arrived, losses, work, task_count, local_hidden, devices
    )
    shared = lax.all_to_all(packed, ("dp", "shard"), 0, 0)
    update, fresh = final_terms(
        shared, task_weights, initial_losses, gradients, entries, shard_count
    )
    return (update, fresh[0, :task_count])


def solution(mesh):
    def step(*arguments):
        return spread(mesh)(*arguments)

    return step


def spread(mesh):
    return jax.shard_map(
        on_device,
        mesh=mesh,
        in_specs=(
            P("dp", None),
            P(None, "shard"),
            P(None, "shard"),
            P("dp", None),
            P("dp", None),
            P(),
            P(),
        ),
        out_specs=(P("dp", "shard"), P()),
        check_vma=False,
    )
```
